32 devices in a mesh: part: 2 (over x), tp: 4 (over z), dp: 4 (over y, core).
Axes of the slice: x: 2, y: 2, z: 4, core: 2. Of those that a mesh axis runs over, the one named last changes fastest.
Arguments:
- x: bfloat16 [4096, 3072], P(('part', 'dp', 'tp')), parts along dimension 0
- w_gate: bfloat16 [6144, 8192], P(('part', 'dp'), 'tp'), parts along dimension 0
- w_up: bfloat16 [6144, 8192], P(('part', 'dp'), 'tp'), parts along dimension 0
- w_down: bfloat16 [16384, 3072], P(('part', 'tp'), 'dp'), parts along dimension 0
- dy: bfloat16 [4096, 3072], P(('part', 'dp', 'tp')), parts along dimension 0
Outputs:
- output 1: bfloat16 [4096, 3072], P(('part', 'dp', 'tp')), parts along dimension 0
- output 2: bfloat16 [4096, 3072], P(('part', 'dp', 'tp')), parts along dimension 0
- output 3: float32 [6144, 8192], P(('part', 'dp'), 'tp'), parts along dimension 0
- output 4: float32 [6144, 8192], P(('part', 'dp'), 'tp'), parts along dimension 0
- output 5: float32 [16384, 3072], P(('part', 'tp'), 'dp'), parts along dimension 0
There are 2 independent parts. The reference program is written for one: setup_inputs(seed, part) draws one part's arguments, and reference() takes and returns one part's arrays. A program takes and returns all parts, laid end to end along the dimension named above; each array names one.
All inputs are finite; a program needn't handle non-finite values.
Results may differ from the reference program's by a relative error of at most 0.001.
Values are sent between devices in bfloat16 or wider.
A program may use at most 1 GiB of HBM per device.

```python
import jax
import jax.numpy as jnp
from jax import lax

D = 3072
FF = 8192
TOKENS_DEV = 128
SHARDS = 16

ROWS = SHARDS * TOKENS_DEV
BLK = min(ROWS, 512)


def setup_inputs(seed: int = 0, part: int = 0) -> dict:
    key = jax.random.fold_in(jax.random.key(seed), part)
    ks = jax.random.split(key, 5)
    x = jax.random.normal(ks[0], (ROWS, D), jnp.float32)
    w_gate = jax.random.normal(ks[1], (D, FF), jnp.float32) * D ** -0.5
    w_up = jax.random.normal(ks[2], (D, FF), jnp.float32) * D ** -0.5
    w_down = jax.random.normal(ks[3], (FF, D), jnp.float32) * FF ** -0.5
    dy = jax.random.normal(ks[4], (ROWS, D), jnp.float32)
    return {'x': x.astype(jnp.bfloat16), 'w_gate': w_gate.astype(jnp.bfloat16), 'w_up': w_up.astype(jnp.bfloat16), 'w_down': w_down.astype(jnp.bfloat16), 'dy': dy.astype(jnp.bfloat16)}


def _block(x, w_gate, w_up, w_down, dy):
    a = jnp.dot(x, w_gate, preferred_element_type=jnp.float32)
    b = jnp.dot(x, w_up, preferred_element_type=jnp.float32)
    sig = jax.nn.sigmoid(a)
    act = a * sig
    h = (act * b).astype(jnp.bfloat16)
    y = (x.astype(jnp.float32) + jnp.dot(h, w_down, preferred_element_type=jnp.float32)).astype(jnp.bfloat16)
    g = jnp.dot(dy, w_down.T, preferred_element_type=jnp.float32)
    da = (g * b * sig * (1.0 + a * (1.0 - sig))).astype(jnp.bfloat16)
    db = (g * act).astype(jnp.bfloat16)
    dx = (dy.astype(jnp.float32) + jnp.dot(da, w_gate.T, preferred_element_type=jnp.float32) + jnp.dot(db, w_up.T, preferred_element_type=jnp.float32)).astype(jnp.bfloat16)
    dw_gate = jnp.dot(x.T, da, preferred_element_type=jnp.float32)
    dw_up = jnp.dot(x.T, db, preferred_element_type=jnp.float32)
    dw_down = jnp.dot(h.T, dy, preferred_element_type=jnp.float32)
    return y, dx, dw_gate, dw_up, dw_down


def reference(x, w_gate, w_up, w_down, dy):
    xb = x.reshape(ROWS // BLK, BLK, D)
    dyb = dy.reshape(ROWS // BLK, BLK, D)

    def step(carry, blk):
        y, dx, dwg, dwu, dwd = _block(blk[0], w_gate, w_up, w_down, blk[1])
        return (carry[0] + dwg, carry[1] + dwu, carry[2] + dwd), (y, dx)

    init = (jnp.zeros((D, FF), jnp.float32), jnp.zeros((D, FF), jnp.float32), jnp.zeros((FF, D), jnp.float32))
    (dwg, dwu, dwd), (y, dx) = lax.scan(step, init, (xb, dyb))
    return (y.reshape(ROWS, D), dx.reshape(ROWS, D), dwg, dwu, dwd)
```

```python
import jax
import jax.numpy as jnp
from jax import lax
from jax.sharding import PartitionSpec as P


OUT_IN = [(0, 1), (3, 2)]
INNER = [(1, 2), (2, 1)]
IN_OUT = [(1, 0), (2, 3)]


def solution(mesh):
    assert mesh.shape['dp'] == 4 and mesh.shape['tp'] == 4
    row_spec = P(('part', 'dp', 'tp'), None)
    win_spec = P(('part', 'dp'), 'tp')
    wout_spec = P(('part', 'tp'), 'dp')
    f32 = jnp.float32
    bf16 = jnp.bfloat16

    def across(t):
        return lax.ppermute(t, 'dp', [(0, 2), (1, 3), (2, 0), (3, 1)])

    def core(t):
        return lax.ppermute(t, 'dp', [(0, 1), (1, 0), (2, 3), (3, 2)])

    def line(t, perm):
        return lax.ppermute(t, 'tp', perm)

    def f(x, wg, wu, wd, dy):
        td, d = x.shape
        dc, fc = wg.shape
        fh = fc // 2
        i = lax.axis_index('dp')
        yy = i // 2
        cc = i % 2
        z = lax.axis_index('tp')
        inner = (z == 1) | (z == 2)

        def by_y(own, other, axis):
            return jnp.where(yy == 0, jnp.concatenate([own, other], axis), jnp.concatenate([other, own], axis))

        def gather_line(t):
            c1 = line(t, IN_OUT)
            c2 = line(t, INNER)
            b1 = line(t, OUT_IN)
            b2 = line(c2, IN_OUT)
            a1 = line(b1, INNER)
            a2 = line(a1, IN_OUT)
            return [jnp.where(inner, a1, a2), jnp.where(inner, b1, b2), jnp.where(inner, c2, c1), t]

        def scatter_line(p):
            pa, pb, pc, pd = p
            r1 = line(pa, OUT_IN)
            rb = line(pb, OUT_IN)
            ra = line(pa + r1, INNER)
            rc = line(pc, OUT_IN)
            rc2 = line(pc + rb, INNER)
            rd = line(pb + ra, IN_OUT)
            return pd + rc + rc2 + rd

        def weight(w, f_axis):
            own = lax.dynamic_slice_in_dim(w, yy * fh, fh, f_axis)
            other = across(lax.dynamic_slice_in_dim(w, (1 - yy) * fh, fh, f_axis))
            p_own, p_other = core(own), core(other)
            k_axis = 1 - f_axis
            shape = (d, fh) if f_axis == 1 else (fh, d)
            out = jnp.zeros(shape, w.dtype)
            for piece, at in ((own, i), (other, i ^ 2), (p_own, i ^ 1), (p_other, i ^ 3)):
                out = lax.dynamic_update_slice_in_dim(out, piece, at * dc, k_axis)
            return out

        def cols(t):
            own = lax.dynamic_slice_in_dim(t, i * dc, dc, 1)
            other = core(lax.dynamic_slice_in_dim(t, (i ^ 1) * dc, dc, 1))
            return jnp.concatenate([own, other], 0)

        def full(t):
            u = by_y(t, across(t), 1)
            return jnp.concatenate([u, core(u)], 0)

        def to_rows(t):
            b = t.reshape(4, td, dc)
            b = jnp.where(cc == 0, b[jnp.array([0, 2, 1, 3])], b[jnp.array([2, 0, 3, 1])])
            v = lax.all_to_all(b, 'dp', 0, 0, tiled=True)
            return v.transpose(1, 0, 2).reshape(td, d)

        def nn(p, q):
            return jnp.dot(p, q, preferred_element_type=f32)

        def nt(p, q):
            return lax.dot_general(p, q, (((1,), (1,)), ((), ())), preferred_element_type=f32)

        def tn(p, q):
            return lax.dot_general(p, q, (((0,), (0,)), ((), ())), preferred_element_type=f32)

        x2 = by_y(x, across(x), 0)
        xs = gather_line(x2)
        wgh = weight(wg, 1)
        wuh = weight(wu, 1)
        dy2 = by_y(dy, across(dy), 0)
        dys = gather_line(dy2)
        wdh = weight(wd, 0)
        a = [nn(t, wgh) for t in xs]
        b = [nn(t, wuh) for t in xs]
        sig = [jax.nn.sigmoid(t) for t in a]
        act = [s * t for s, t in zip(sig, a)]
        h = [full((s * t).astype(bf16)) for s, t in zip(act, b)]
        y_s = scatter_line([nn(t, wd) for t in h])
        xc = [cols(t) for t in xs]
        y = to_rows((xc[3].astype(f32) + y_s).astype(bf16))
        g = [nt(t, wdh) for t in dys]
        da = [full((gg * bb * s * (1.0 + aa * (1.0 - s))).astype(bf16)) for gg, bb, s, aa in zip(g, b, sig, a)]
        db = [full((gg * t).astype(bf16)) for gg, t in zip(g, act)]
        dx_s = scatter_line([nt(p, wg) + nt(q, wu) for p, q in zip(da, db)])
        dyc = [cols(t) for t in dys]
        dx = to_rows((dyc[3].astype(f32) + dx_s).astype(bf16))
        dwd = tn(jnp.concatenate(h), jnp.concatenate(dyc))
        xcc = jnp.concatenate(xc)
        dwg = tn(xcc, jnp.concatenate(da))
        dwu = tn(xcc, jnp.concatenate(db))
        return y, dx, dwg, dwu, dwd

    return jax.shard_map(f, mesh=mesh, in_specs=(row_spec, win_spec, win_spec, wout_spec, row_spec), out_specs=(row_spec, row_spec, win_spec, win_spec, wout_spec), check_vma=False)
```
